128 devices in a mesh: py: 4 (over y), px: 8 (over z_lo, x), pz: 4 (over z_hi, core).
Axes of the slice: x: 4, y: 4, z: 4 (z_hi: 2, z_lo: 2; z = z_hi * 2 + z_lo), core: 2. Of those that a mesh axis runs over, the one named last changes fastest.
Arguments:
- starting_state: float32 [512, 32, 128, 128], P('py', 'px', 'pz'), may hold values from 0.5 to 2
- scaled_conductivity: float32 [512, 32, 128, 128], P('py', 'px', 'pz'), may hold values from 0.03 to 0.15
- scaled_heat_supply: float32 [512, 32, 128, 128], P('py', 'px', 'pz'), may hold values from -0.2 to 0.2
Outputs:
- normalised_result: float32 [512, 32, 128, 128], P('py', 'px', 'pz')
- temperature_end: float32 [512, 32, 128, 128], P('py', 'px', 'pz')
The draws below stay inside these ranges and needn't reach their ends.
All inputs are finite; a program needn't handle non-finite values.
Results may differ from the reference program's by a relative error of at most 0.00002.
Values sent between devices are 32-bit elements; how exact they have to be, the bound alone decides.
A program may use at most 128 MiB of HBM per device.

```python
import jax
import jax.numpy as jnp
from jax import lax

GRID_DEPTH = 512
GRID_WIDTH = 32
GRID_HEIGHT = 128
SAMPLE_TOTAL = 128
STEPS = 4


def block_levels(rng, shape, split, low, high):
    def one(position, parts):
        heights = jax.random.uniform(jax.random.fold_in(jax.random.fold_in(rng, 6), position), (parts,), jnp.float32, low / len(split), high / len(split))
        return jnp.repeat(jnp.exp(heights), shape[position] // parts).reshape((-1,) + (1,) * (len(shape) - position - 1))

    level = one(*split[0])
    for cut in split[1:]:
        level = level * one(*cut)
    return level


def setup_inputs(seed: int = 0) -> dict:
    keys = jax.random.split(jax.random.key(seed), 4)
    return {
        "starting_state": jnp.clip(0.5 + 1.5 * jax.random.uniform(keys[0], (GRID_DEPTH, GRID_WIDTH, GRID_HEIGHT, SAMPLE_TOTAL), jnp.float32) ** block_levels(keys[0], (GRID_DEPTH, GRID_WIDTH, GRID_HEIGHT, SAMPLE_TOTAL), ((0, 4), (1, 8), (2, 4)), -0.2, 0.2), 0.5, 2.0),
        "scaled_conductivity": jnp.clip(0.03 + 0.120000007 * jax.random.uniform(keys[1], (GRID_DEPTH, GRID_WIDTH, GRID_HEIGHT, SAMPLE_TOTAL), jnp.float32) ** block_levels(keys[1], (GRID_DEPTH, GRID_WIDTH, GRID_HEIGHT, SAMPLE_TOTAL), ((0, 4), (1, 8), (2, 4)), -0.2, 0.2), 0.03, 0.15),
        "scaled_heat_supply": jnp.clip(jax.random.uniform(keys[2], (GRID_DEPTH, GRID_WIDTH, GRID_HEIGHT, SAMPLE_TOTAL), jnp.float32, -0.2, 0.2) * block_levels(keys[2], (GRID_DEPTH, GRID_WIDTH, GRID_HEIGHT, SAMPLE_TOTAL), ((0, 4), (1, 8), (2, 4)), -0.4, 0.0), -0.2, 0.2),
    }


def interior_points(values, dims):
    for coordinate_axis in dims:
        values = lax.slice_in_dim(values, 1, values.shape[coordinate_axis] - 1, axis=coordinate_axis)
    return values

def boundary_layer(values, coordinate_axis, start, dims):
    others = [other for other in dims if other != coordinate_axis]
    values = interior_points(values, others)
    return lax.slice_in_dim(values, start, start + values.shape[coordinate_axis] - 2, axis=coordinate_axis)

def conduction_timestep(framed_thermal_lattice, scaled_conductivity, scaled_heat_supply):
    central_point = interior_points(framed_thermal_lattice, (0, 1, 2))
    preceding_neighbour = [boundary_layer(framed_thermal_lattice, coordinate_axis, 0, (0, 1, 2)) for coordinate_axis in (0, 1, 2)]
    following_neighbour = [boundary_layer(framed_thermal_lattice, coordinate_axis, 2, (0, 1, 2)) for coordinate_axis in (0, 1, 2)]
    spread = preceding_neighbour[0] + following_neighbour[0] + preceding_neighbour[1] + following_neighbour[1] + preceding_neighbour[2] + following_neighbour[2] - 6.0 * central_point
    return central_point + scaled_conductivity * spread + scaled_heat_supply

def reference(starting_state, scaled_conductivity, scaled_heat_supply):
    for step in range(STEPS):
        starting_state = conduction_timestep(jnp.pad(starting_state, ((1, 1), (1, 1), (1, 1), (0, 0)), mode='constant'), scaled_conductivity, scaled_heat_supply)
    row_average = lax.optimization_barrier(jnp.mean(starting_state, axis=1, keepdims=True))
    deviation_rows = starting_state - row_average
    line_variance = lax.optimization_barrier(jnp.mean(deviation_rows * deviation_rows, axis=1, keepdims=True))
    normalised_result = deviation_rows * lax.rsqrt(line_variance + 0.0001)
    return (normalised_result, starting_state)
```

```python
import jax
import jax.numpy as jnp
from jax import lax
from jax.experimental import pallas as pl
from jax.experimental.pallas import tpu as pltpu
from jax.sharding import PartitionSpec as P

STEPS = 4
NC = 8
MESH = pl.DeviceIdType.MESH
F32 = jnp.float32


def merge(sum_a, square_a, count_a, sum_b, square_b, count_b):
    gap = sum_a * (1.0 / count_a) - sum_b * (1.0 / count_b)
    weight = count_a * count_b / (count_a + count_b)
    return sum_a + sum_b, square_a + square_b + gap * gap * weight


def main_kernel(
    u_in, k_in, q_in, u_out, f_out,
    field, cond, supply, zsend, zrecv, part, full, ring, across,
    load_sem, out_sem, xs_sem, xr_sem, zs_sem, zr_sem, ys_sem, yr_sem, ss_sem, sr_sem,
):
    rows, cols, height, lanes = u_in.shape
    chunk = rows // NC
    half = chunk // 2
    py, px, pz = lax.axis_index("py"), lax.axis_index("px"), lax.axis_index("pz")
    ny, nx, nz = lax.axis_size("py"), lax.axis_size("px"), lax.axis_size("pz")
    groups = 4
    xq = lax.rem(px, groups)
    zq = px - xq
    right = {"px": zq + lax.rem(xq + 1, groups)}
    left = {"px": zq + lax.rem(xq + groups - 1, groups)}
    partner = {"px": lax.rem(px + groups, nx)}
    x_after, x_before = lax.rem(xq + 1, groups), lax.rem(xq + groups - 1, groups)
    x_far = lax.rem(xq + 2, groups)

    has = {
        ("x", 0): px > 0, ("x", 1): px < nx - 1,
        ("y", 0): py > 0, ("y", 1): py < ny - 1,
        ("z", 0): pz > 0, ("z", 1): pz < nz - 1,
    }
    peer = {
        ("x", 0): {"px": px - 1}, ("x", 1): {"px": px + 1},
        ("y", 0): {"py": py - 1}, ("y", 1): {"py": py + 1},
        ("z", 0): {"pz": pz - 1}, ("z", 1): {"pz": pz + 1},
    }

    barrier = pltpu.get_barrier_semaphore()
    count = jnp.int32(3)
    for key in has:
        count = count + has[key].astype(jnp.int32)

        @pl.when(has[key])
        def _():
            pl.semaphore_signal(barrier, inc=1, device_id=peer[key], device_id_type=MESH)

    for other in (right, left, partner):
        pl.semaphore_signal(barrier, inc=1, device_id=other, device_id_type=MESH)

    def load(c, which):
        span = pl.ds(c * chunk, chunk)
        if which == 0:
            return pltpu.make_async_copy(
                u_in.at[span], field.at[0, pl.ds(c * chunk + 1, chunk), pl.ds(1, cols)], load_sem.at[0, c]
            )
        source, target = ((k_in, cond), (q_in, supply))[which - 1]
        return pltpu.make_async_copy(source.at[span], target.at[span], load_sem.at[which, c])

    def remote(src, dst, send, recv, device):
        return pltpu.make_async_remote_copy(
            src_ref=src, dst_ref=dst, send_sem=send, recv_sem=recv, device_id=device, device_id_type=MESH
        )

    def x_copy(slot, c, side, first=False):
        span = pl.ds(c * chunk, chunk)
        padded = pl.ds(c * chunk + 1, chunk)
        edge = 0 if side == 0 else cols - 1
        src = u_in.at[span, edge] if first else field.at[slot, padded, edge + 1]
        return remote(
            src, field.at[slot, padded, cols + 1 if side == 0 else 0],
            xs_sem.at[side, slot, c], xr_sem.at[1 - side, slot, c], peer["x", side],
        )

    def x_arrival(slot, c, side):
        padded = pl.ds(c * chunk + 1, chunk)
        dst = field.at[slot, padded, 0 if side == 0 else cols + 1]
        return remote(dst, dst, xs_sem.at[side, slot, c], xr_sem.at[side, slot, c], peer["x", side])

    def z_copy(slot, c, side):
        span = pl.ds(c * chunk, chunk)
        return remote(
            zsend.at[slot, side, span], zrecv.at[slot, 1 - side, span],
            zs_sem.at[side, slot, c], zr_sem.at[1 - side, slot, c], peer["z", side],
        )

    def z_arrival(slot, c, side):
        dst = zrecv.at[slot, side, pl.ds(c * chunk, chunk)]
        return remote(dst, dst, zs_sem.at[side, slot, c], zr_sem.at[side, slot, c], peer["z", side])

    def y_copy(slot, side, first=False):
        inner = pl.ds(1, cols)
        row = 0 if side == 0 else rows - 1
        src = u_in.at[row] if first else field.at[slot, row + 1, inner]
        return remote(
            src, field.at[slot, rows + 1 if side == 0 else 0, inner],
            ys_sem.at[side, slot], yr_sem.at[1 - side, slot], peer["y", side],
        )

    def y_arrival(slot, side):
        dst = field.at[slot, 0 if side == 0 else rows + 1, pl.ds(1, cols)]
        return remote(dst, dst, ys_sem.at[side, slot], yr_sem.at[side, slot], peer["y", side])

    for which in range(3):
        @pl.loop(0, NC)
        def _(c):
            load(c, which).start()

    pl.semaphore_wait(barrier, count)

    for side in range(2):
        @pl.when(has["x", side])
        def _():
            @pl.loop(0, NC)
            def _(c):
                x_copy(0, c, side, first=True).start()

        @pl.when(has["y", side])
        def _():
            y_copy(0, side, first=True).start()

    zero_column = jnp.zeros((height, lanes), F32)
    zero_edge = jnp.zeros((cols, lanes), F32)
    for side in range(2):
        @pl.when(jnp.logical_not(has["x", side]))
        def _():
            @pl.loop(0, rows)
            def _(y):
                for slot in range(2):
                    field[slot, y + 1, 0 if side == 0 else cols + 1] = zero_column

        @pl.when(jnp.logical_not(has["y", side]))
        def _():
            for slot in range(2):
                for x in range(cols):
                    field[slot, 0 if side == 0 else rows + 1, x + 1] = zero_column

        @pl.when(jnp.logical_not(has["z", side]))
        def _():
            @pl.loop(0, rows)
            def _(y):
                for slot in range(2):
                    zrecv[slot, side, y] = zero_edge

    def pack(slot, y, x, value):
        zsend[slot, 0, y, x : x + 1] = value[0:1]
        zsend[slot, 1, y, x : x + 1] = value[height - 1 : height]

    @pl.loop(0, NC)
    def _(c):
        load(c, 0).wait()

        @pl.loop(0, chunk)
        def _(r):
            y = c * chunk + r
            for x in range(cols):
                pack(0, y, x, field[0, y + 1, x + 1])

        for side in range(2):
            @pl.when(has["z", side])
            def _():
                z_copy(0, c, side).start()

    row_index = lax.broadcasted_iota(jnp.int32, (height, lanes), 0)
    at_low, at_high = row_index == 0, row_index == height - 1

    def compute(step, c):
        src, dst = step % 2, (step + 1) % 2
        if step == 0:
            load(c, 1).wait()
            load(c, 2).wait()
        for side in range(2):
            @pl.when(has["x", side])
            def _():
                x_arrival(src, c, side).wait_recv()
                if step >= 1:
                    x_copy(dst, c, side).wait_send()

            @pl.when(has["z", side])
            def _():
                z_arrival(src, c, side).wait_recv()
                if step >= 1:
                    z_copy(dst, c, side).wait_send()

            @pl.when(jnp.logical_and(has["y", side], c == (0 if side == 0 else NC - 1)))
            def _():
                y_arrival(src, side).wait_recv()
                if step >= 1:
                    y_copy(dst, side).wait_send()

        @pl.loop(0, chunk)
        def _(r):
            y = c * chunk + r
            fresh = []
            for x in range(cols):
                here = field[src, y + 1, x + 1]
                below = jnp.where(at_low, zrecv[src, 0, y, x : x + 1], pltpu.roll(here, 1, 0))
                above = jnp.where(at_high, zrecv[src, 1, y, x : x + 1], pltpu.roll(here, height - 1, 0))
                spread = (
                    field[src, y, x + 1] + field[src, y + 2, x + 1]
                    + field[src, y + 1, x] + field[src, y + 1, x + 2]
                    + below + above - 6.0 * here
                )
                value = here + cond[y, x] * spread + supply[y, x]
                field[dst, y + 1, x + 1] = value
                if step < STEPS - 1:
                    pack(dst, y, x, value)
                fresh.append(value)
            if step == STEPS - 1:
                total = (fresh[0] + fresh[1]) + (fresh[2] + fresh[3])
                middle = total * (1.0 / cols)
                square = None
                for value in fresh:
                    away = value - middle
                    square = away * away if square is None else square + away * away
                for g in range(groups):
                    part[g, 0, y] = total[8 * g : 8 * g + 8]
                    part[g, 1, y] = square[8 * g : 8 * g + 8]

        if step < STEPS - 1:
            for side in range(2):
                @pl.when(has["x", side])
                def _():
                    x_copy(dst, c, side).start()

                @pl.when(has["z", side])
                def _():
                    z_copy(dst, c, side).start()

                @pl.when(jnp.logical_and(has["y", side], c == (0 if side == 0 else NC - 1)))
                def _():
                    y_copy(dst, side).start()

    for step in range(STEPS - 1):
        @pl.loop(0, NC)
        def _(c):
            compute(step, c)

    last = STEPS % 2

    def u_store(c):
        return pltpu.make_async_copy(
            field.at[last, pl.ds(c * chunk + 1, chunk), pl.ds(1, cols)],
            u_out.at[pl.ds(c * chunk, chunk)], out_sem.at[0, c],
        )

    def f_store(c):
        span = pl.ds(c * chunk, chunk)
        return pltpu.make_async_copy(full.at[:, :, span], f_out.at[:, :, span], out_sem.at[1, c])

    def plus(c):
        return pl.ds(c * chunk, half)

    def minus(c):
        return pl.ds(c * chunk + half, half)

    def whole(c):
        return pl.ds(c * chunk, chunk)

    def stat(kind, c):
        send, recv = ss_sem.at[kind, c], sr_sem.at[kind, c]
        if kind == 0:
            return remote(part.at[x_far, :, plus(c)], ring.at[0, :, c], send, recv, right)
        if kind == 1:
            return remote(part.at[x_far, :, minus(c)], ring.at[1, :, c], send, recv, left)
        if kind == 2:
            return remote(part.at[x_after, :, minus(c)], ring.at[2, :, c], send, recv, right)
        if kind == 3:
            return remote(part.at[x_before, :, plus(c)], ring.at[3, :, c], send, recv, left)
        if kind == 4:
            return remote(part.at[x_after, :, plus(c)], ring.at[4, :, c], send, recv, right)
        if kind == 5:
            return remote(part.at[x_before, :, minus(c)], ring.at[5, :, c], send, recv, left)
        if kind == 6:
            return remote(part.at[xq, :, whole(c)], across.at[:, whole(c)], send, recv, partner)
        if kind == 7:
            return remote(full.at[xq, :, whole(c)], full.at[xq, :, whole(c)], send, recv, right)
        if kind == 8:
            return remote(full.at[xq, :, whole(c)], full.at[xq, :, whole(c)], send, recv, left)
        if kind == 9:
            return remote(full.at[x_before, :, plus(c)], full.at[x_before, :, plus(c)], send, recv, right)
        return remote(full.at[x_after, :, minus(c)], full.at[x_after, :, minus(c)], send, recv, left)

    def stat_arrival(kind, c):
        send, recv = ss_sem.at[kind, c], sr_sem.at[kind, c]
        if kind < 6:
            dst = ring.at[kind, :, c]
        elif kind == 6:
            dst = across.at[:, whole(c)]
        elif kind == 7:
            dst = full.at[x_before, :, whole(c)]
        elif kind == 8:
            dst = full.at[x_after, :, whole(c)]
        elif kind == 9:
            dst = full.at[x_far, :, plus(c)]
        else:
            dst = full.at[x_far, :, minus(c)]
        return remote(dst, dst, send, recv, partner)

    def stage_a(c):
        u_store(c).start()
        for kind in range(4):
            stat(kind, c).start()

    def stage_b(c):
        for kind, owner, offset in ((0, x_after, 0), (1, x_before, half)):
            stat_arrival(kind, c).wait_recv()
            span = pl.ds(c * chunk + offset, half)
            total, square = merge(
                part[owner, 0, span], part[owner, 1, span], 4.0, ring[kind, 0, c], ring[kind, 1, c], 4.0
            )
            part[owner, 0, span] = total
            part[owner, 1, span] = square
            stat(4 + kind, c).start()

    def stage_c(c):
        for kind in (2, 3, 4, 5):
            stat_arrival(kind, c).wait_recv()
        for near, far, offset in ((3, 4, 0), (2, 5, half)):
            span = pl.ds(c * chunk + offset, half)
            total, square = merge(
                part[xq, 0, span], part[xq, 1, span], 4.0, ring[near, 0, c], ring[near, 1, c], 4.0
            )
            total, square = merge(total, square, 8.0, ring[far, 0, c], ring[far, 1, c], 8.0)
            part[xq, 0, span] = total
            part[xq, 1, span] = square
        stat(6, c).start()

    def stage_d(c):
        stat_arrival(6, c).wait_recv()
        for offset in (0, half):
            span = pl.ds(c * chunk + offset, half)
            total, square = merge(part[xq, 0, span], part[xq, 1, span], 16.0, across[0, span], across[1, span], 16.0)
            full[xq, 0, span] = total * (1.0 / 32.0)
            full[xq, 1, span] = lax.rsqrt(square * (1.0 / 32.0) + 0.0001)
        stat(7, c).start()
        stat(8, c).start()

    def stage_e(c):
        stat_arrival(7, c).wait_recv()
        stat(9, c).start()
        stat_arrival(8, c).wait_recv()
        stat(10, c).start()

    def stage_g(c):
        stat_arrival(9, c).wait_recv()
        stat_arrival(10, c).wait_recv()
        f_store(c).start()

    def first_stage(c):
        compute(STEPS - 1, c)
        stage_a(c)

    stages = (first_stage, stage_b, stage_c, stage_d, stage_e, stage_g)

    @pl.loop(0, NC + len(stages) - 1)
    def _(k):
        for delay, stage in enumerate(stages):
            @pl.when(jnp.logical_and(k >= delay, k < NC + delay))
            def _():
                stage(k - delay)

    @pl.loop(0, NC)
    def _(c):
        for side in range(2):
            @pl.when(has["x", side])
            def _():
                x_copy((STEPS - 1) % 2, c, side).wait_send()

            @pl.when(has["z", side])
            def _():
                z_copy((STEPS - 1) % 2, c, side).wait_send()

        for kind in range(11):
            stat(kind, c).wait_send()
        u_store(c).wait()
        f_store(c).wait()

    for side in range(2):
        @pl.when(has["y", side])
        def _():
            y_copy((STEPS - 1) % 2, side).wait_send()


def finish_kernel(u_ref, f_ref, norm_ref, end_ref):
    value = u_ref[...]
    end_ref[...] = value
    for g in range(4):
        band = slice(8 * g, 8 * g + 8)
        norm_ref[:, :, band] = (value[:, :, band] - f_ref[g, 0][:, None]) * f_ref[g, 1][:, None]


def body(u, k, q):
    rows, cols, height, lanes = u.shape
    dma = pltpu.SemaphoreType.DMA
    moved, stats = pl.pallas_call(
        main_kernel,
        out_shape=(
            jax.ShapeDtypeStruct(u.shape, F32),
            jax.ShapeDtypeStruct((4, 2, rows, 8, lanes), F32),
        ),
        in_specs=[pl.BlockSpec(memory_space=pl.ANY)] * 3,
        out_specs=[pl.BlockSpec(memory_space=pl.ANY)] * 2,
        scratch_shapes=[
            pltpu.VMEM((2, rows + 2, cols + 2, height, lanes), F32),
            pltpu.VMEM(u.shape, F32),
            pltpu.VMEM(u.shape, F32),
            pltpu.VMEM((2, 2, rows, cols, lanes), F32),
            pltpu.VMEM((2, 2, rows, cols, lanes), F32),
            pltpu.VMEM((4, 2, rows, 8, lanes), F32),
            pltpu.VMEM((4, 2, rows, 8, lanes), F32),
            pltpu.VMEM((6, 2, NC, rows // NC // 2, 8, lanes), F32),
            pltpu.VMEM((2, rows, 8, lanes), F32),
            dma((3, NC)), dma((2, NC)),
            dma((2, 2, NC)), dma((2, 2, NC)), dma((2, 2, NC)), dma((2, 2, NC)),
            dma((2, 2)), dma((2, 2)), dma((11, NC)), dma((11, NC)),
        ],
        compiler_params=pltpu.CompilerParams(
            collective_id=0, has_side_effects=True, vmem_limit_bytes=62 * 1024 * 1024
        ),
        name="heat_steps",
    )(u, k, q)
    tile = 8
    block = pl.BlockSpec((tile, cols, height, lanes), lambda i: (i, 0, 0, 0))
    return pl.pallas_call(
        finish_kernel,
        grid=(rows // tile,),
        out_shape=(jax.ShapeDtypeStruct(u.shape, F32),) * 2,
        in_specs=[block, pl.BlockSpec((4, 2, tile, 8, lanes), lambda i: (0, 0, i, 0, 0))],
        out_specs=[block, block],
        name="centre_and_scale",
    )(moved, stats)


def solution(mesh):
    placed = P("py", "px", "pz", None)
    return jax.shard_map(
        body, mesh=mesh, in_specs=(placed, placed, placed), out_specs=(placed, placed), check_vma=False
    )
```

```python
import jax
import jax.numpy as jnp
from jax import lax
from jax.experimental import pallas as pl
from jax.experimental.pallas import tpu as pltpu
from jax.sharding import PartitionSpec as P

STEPS = 4
NC = 8
FIRST = 5
MESH = pl.DeviceIdType.MESH
F32 = jnp.float32


def merge(sum_a, square_a, count_a, sum_b, square_b, count_b):
    gap = sum_a * (1.0 / count_a) - sum_b * (1.0 / count_b)
    weight = count_a * count_b / (count_a + count_b)
    return sum_a + sum_b, square_a + square_b + gap * gap * weight


def main_kernel(
    u_in, k_in, q_in, u_out, f_out,
    field, cond, supply, zsend, zrecv, part, full, ring, across, halves, passing,
    load_sem, out_sem, ps_sem, pr_sem, xs_sem, xr_sem, zs_sem, zr_sem, ys_sem, yr_sem, ss_sem, sr_sem,
):
    rows, cols, height, lanes = u_in.shape
    chunk = rows // NC
    half = chunk // 2
    py, px, pz = lax.axis_index("py"), lax.axis_index("px"), lax.axis_index("pz")
    ny, nx, nz = lax.axis_size("py"), lax.axis_size("px"), lax.axis_size("pz")
    groups = 4
    xq = lax.rem(px, groups)
    zq = px - xq
    right = {"px": zq + lax.rem(xq + 1, groups)}
    left = {"px": zq + lax.rem(xq + groups - 1, groups)}
    partner = {"px": lax.rem(px + groups, nx)}
    x_after, x_before = lax.rem(xq + 1, groups), lax.rem(xq + groups - 1, groups)
    x_far = lax.rem(xq + 2, groups)

    has = {
        ("x", 0): px > 0, ("x", 1): px < nx - 1,
        ("y", 0): py > 0, ("y", 1): py < ny - 1,
        ("z", 0): pz > 0, ("z", 1): pz < nz - 1,
    }
    peer = {
        ("x", 0): {"px": px - 1}, ("x", 1): {"px": px + 1},
        ("y", 0): {"py": py - 1}, ("y", 1): {"py": py + 1},
        ("z", 0): {"pz": pz - 1}, ("z", 1): {"pz": pz + 1},
    }

    barrier = pltpu.get_barrier_semaphore()
    count = jnp.int32(3)
    for key in has:
        count = count + has[key].astype(jnp.int32)

        @pl.when(has[key])
        def _():
            pl.semaphore_signal(barrier, inc=1, device_id=peer[key], device_id_type=MESH)

    for other in (right, left, partner):
        pl.semaphore_signal(barrier, inc=1, device_id=other, device_id_type=MESH)

    def load(c, which):
        span = pl.ds(c * chunk, chunk)
        if which == 0:
            return pltpu.make_async_copy(
                u_in.at[span], field.at[0, pl.ds(c * chunk + 1, chunk), pl.ds(1, cols)], load_sem.at[0, c]
            )
        source, target = ((k_in, cond), (q_in, supply))[which - 1]
        return pltpu.make_async_copy(source.at[span], target.at[span], load_sem.at[which, c])

    def remote(src, dst, send, recv, device):
        return pltpu.make_async_remote_copy(
            src_ref=src, dst_ref=dst, send_sem=send, recv_sem=recv, device_id=device, device_id_type=MESH
        )

    def x_copy(slot, c, side, first=False):
        span = pl.ds(c * chunk, chunk)
        padded = pl.ds(c * chunk + 1, chunk)
        edge = 0 if side == 0 else cols - 1
        src = u_in.at[span, edge] if first else field.at[slot, padded, edge + 1]
        return remote(
            src, field.at[slot, padded, cols + 1 if side == 0 else 0],
            xs_sem.at[side, slot, c], xr_sem.at[1 - side, slot, c], peer["x", side],
        )

    middle = nx // 2
    at_seam = (px == middle, px == middle - 1)
    carries = (px == 0, px == nx - 1)

    def odd(c):
        return lax.rem(c, 2) == 1

    def x_detour(slot, c, side, step):
        edge = 0 if side == 0 else cols - 1
        if step == 0:
            src = u_in.at[pl.ds(c * chunk, chunk), edge]
        else:
            src = field.at[slot, pl.ds(c * chunk + 1, chunk), edge + 1]
        return remote(
            src, passing.at[step, lax.div(c, 2)],
            xs_sem.at[side, slot, c], pr_sem.at[step, lax.div(c, 2)], partner,
        )

    def x_start(step, c, side):
        slot = step % 2
        detour = jnp.logical_and(at_seam[side], odd(c))

        @pl.when(detour)
        def _():
            x_detour(slot, c, side, step).start()

        @pl.when(jnp.logical_not(detour))
        def _():
            x_copy(slot, c, side, step == 0).start()

    def pass_on(step, c, side):
        here, slot = passing.at[step, lax.div(c, 2)], step % 2
        return remote(
            here, field.at[slot, pl.ds(c * chunk + 1, chunk), cols + 1 if side == 0 else 0],
            ps_sem.at[step, lax.div(c, 2)], xr_sem.at[1 - side, slot, c],
            {"px": middle - 1 if side == 0 else middle},
        )

    def relay(step, c):
        here = passing.at[step, lax.div(c, 2)]
        for side in range(2):
            @pl.when(jnp.logical_and(carries[side], odd(c)))
            def _():
                remote(
                    here, here, ps_sem.at[step, lax.div(c, 2)], pr_sem.at[step, lax.div(c, 2)], partner
                ).wait_recv()
                pass_on(step, c, side).start()

    def x_arrival(slot, c, side):
        padded = pl.ds(c * chunk + 1, chunk)
        dst = field.at[slot, padded, 0 if side == 0 else cols + 1]
        return remote(dst, dst, xs_sem.at[side, slot, c], xr_sem.at[side, slot, c], peer["x", side])

    def z_copy(slot, c, side):
        span = pl.ds(c * chunk, chunk)
        return remote(
            zsend.at[slot, side, span], zrecv.at[slot, 1 - side, span],
            zs_sem.at[side, slot, c], zr_sem.at[1 - side, slot, c], peer["z", side],
        )

    def z_arrival(slot, c, side):
        dst = zrecv.at[slot, side, pl.ds(c * chunk, chunk)]
        return remote(dst, dst, zs_sem.at[side, slot, c], zr_sem.at[side, slot, c], peer["z", side])

    def y_copy(slot, side, first=False):
        inner = pl.ds(1, cols)
        row = 0 if side == 0 else rows - 1
        src = u_in.at[row] if first else field.at[slot, row + 1, inner]
        return remote(
            src, field.at[slot, rows + 1 if side == 0 else 0, inner],
            ys_sem.at[side, slot], yr_sem.at[1 - side, slot], peer["y", side],
        )

    def y_arrival(slot, side):
        dst = field.at[slot, 0 if side == 0 else rows + 1, pl.ds(1, cols)]
        return remote(dst, dst, ys_sem.at[side, slot], yr_sem.at[side, slot], peer["y", side])

    for which in range(3):
        @pl.loop(0, NC)
        def _(c):
            load(c, which).start()

    pl.semaphore_wait(barrier, count)

    for side in range(2):
        @pl.when(has["x", side])
        def _():
            @pl.loop(0, NC)
            def _(c):
                x_start(0, c, side)

        @pl.when(has["y", side])
        def _():
            y_copy(0, side, first=True).start()

    zero_column = jnp.zeros((height, lanes), F32)
    zero_edge = jnp.zeros((cols, lanes), F32)
    for side in range(2):
        @pl.when(jnp.logical_not(has["x", side]))
        def _():
            @pl.loop(0, rows)
            def _(y):
                for slot in range(2):
                    field[slot, y + 1, 0 if side == 0 else cols + 1] = zero_column

        @pl.when(jnp.logical_not(has["y", side]))
        def _():
            for slot in range(2):
                for x in range(cols):
                    field[slot, 0 if side == 0 else rows + 1, x + 1] = zero_column

        @pl.when(jnp.logical_not(has["z", side]))
        def _():
            @pl.loop(0, rows)
            def _(y):
                for slot in range(2):
                    zrecv[slot, side, y] = zero_edge

    def pack(slot, y, x, value):
        zsend[slot, 0, y, x : x + 1] = value[0:1]
        zsend[slot, 1, y, x : x + 1] = value[height - 1 : height]

    @pl.loop(0, NC)
    def _(c):
        load(c, 0).wait()

        @pl.loop(0, chunk)
        def _(r):
            y = c * chunk + r
            for x in range(cols):
                pack(0, y, x, field[0, y + 1, x + 1])

        for side in range(2):
            @pl.when(has["z", side])
            def _():
                z_copy(0, c, side).start()

    row_index = lax.broadcasted_iota(jnp.int32, (height, lanes), 0)
    at_low, at_high = row_index == 0, row_index == height - 1

    def compute(step, c):
        src, dst = step % 2, (step + 1) % 2
        if step == 0:
            load(c, 1).wait()
            load(c, 2).wait()
            relay(0, c)
        for side in range(2):
            @pl.when(has["x", side])
            def _():
                x_arrival(src, c, side).wait_recv()
                if step >= 1:
                    x_copy(dst, c, side).wait_send()

            @pl.when(has["z", side])
            def _():
                z_arrival(src, c, side).wait_recv()
                if step >= 1:
                    z_copy(dst, c, side).wait_send()

            @pl.when(jnp.logical_and(has["y", side], c == (0 if side == 0 else NC - 1)))
            def _():
                y_arrival(src, side).wait_recv()
                if step >= 1:
                    y_copy(dst, side).wait_send()

        @pl.loop(0, chunk)
        def _(r):
            y = c * chunk + r
            fresh = []
            for x in range(cols):
                here = field[src, y + 1, x + 1]
                below = jnp.where(at_low, zrecv[src, 0, y, x : x + 1], pltpu.roll(here, 1, 0))
                above = jnp.where(at_high, zrecv[src, 1, y, x : x + 1], pltpu.roll(here, height - 1, 0))
                spread = (
                    field[src, y, x + 1] + field[src, y + 2, x + 1]
                    + field[src, y + 1, x] + field[src, y + 1, x + 2]
                    + below + above - 6.0 * here
                )
                value = here + cond[y, x] * spread + supply[y, x]
                field[dst, y + 1, x + 1] = value
                if step < STEPS - 1:
                    pack(dst, y, x, value)
                fresh.append(value)
            if step == STEPS - 1:
                total = (fresh[0] + fresh[1]) + (fresh[2] + fresh[3])
                middle = total * (1.0 / cols)
                square = None
                for value in fresh:
                    away = value - middle
                    square = away * away if square is None else square + away * away
                for g in range(groups):
                    part[g, 0, y] = total[8 * g : 8 * g + 8]
                    part[g, 1, y] = square[8 * g : 8 * g + 8]

        if step < STEPS - 1:
            for side in range(2):
                @pl.when(has["x", side])
                def _():
                    x_start(step + 1, c, side)

                @pl.when(has["z", side])
                def _():
                    z_copy(dst, c, side).start()

                @pl.when(jnp.logical_and(has["y", side], c == (0 if side == 0 else NC - 1)))
                def _():
                    y_copy(dst, side).start()

            @pl.when(c > 0)
            def _():
                relay(step + 1, c - 1)

        if step >= 1:
            @pl.when(c == 0)
            def _():
                relay(step, NC - 1)

    for step in range(STEPS - 1):
        @pl.loop(0, NC)
        def _(c):
            compute(step, c)

    last = STEPS % 2

    def u_store(c):
        return pltpu.make_async_copy(
            field.at[last, pl.ds(c * chunk + 1, chunk), pl.ds(1, cols)],
            u_out.at[pl.ds(c * chunk, chunk)], out_sem.at[0, c],
        )

    def f_store(c):
        span = pl.ds(c * chunk, chunk)
        return pltpu.make_async_copy(full.at[:, :, span], f_out.at[:, :, span], out_sem.at[1, c])

    lower = lax.div(px, groups)

    def span_of(c, mine):
        if mine:
            return c * chunk + lower * half, half // 2
        return c * chunk, half

    def plus(c, mine):
        start, size = span_of(c, mine)
        return pl.ds(start, size)

    def minus(c, mine):
        start, size = span_of(c, mine)
        return pl.ds(start + size, size)

    def whole(c, mine):
        start, size = span_of(c, mine)
        return pl.ds(start, 2 * size)

    def other(c):
        return pl.ds(c * chunk + (1 - lower) * half, half)

    def landing(kind, c, mine):
        return ring.at[kind, :, c, pl.ds(0, half // 2)] if mine else ring.at[kind, :, c]

    def stat(kind, c, mine):
        send, recv = ss_sem.at[kind, c], sr_sem.at[kind, c]
        if kind == 0:
            return remote(part.at[x_far, :, plus(c, mine)], landing(0, c, mine), send, recv, right)
        if kind == 1:
            return remote(part.at[x_far, :, minus(c, mine)], landing(1, c, mine), send, recv, left)
        if kind == 2:
            return remote(part.at[x_after, :, minus(c, mine)], landing(2, c, mine), send, recv, right)
        if kind == 3:
            return remote(part.at[x_before, :, plus(c, mine)], landing(3, c, mine), send, recv, left)
        if kind == 4:
            return remote(part.at[x_after, :, plus(c, mine)], landing(4, c, mine), send, recv, right)
        if kind == 5:
            return remote(part.at[x_before, :, minus(c, mine)], landing(5, c, mine), send, recv, left)
        if kind == 6:
            if mine:
                return remote(part.at[:, :, other(c)], halves.at[:, :, pl.ds(c * half, half)], send, recv, partner)
            return remote(part.at[xq, :, whole(c, mine)], across.at[:, pl.ds((c - FIRST) * chunk, chunk)], send, recv, partner)
        if kind == 7:
            return remote(full.at[xq, :, whole(c, mine)], full.at[xq, :, whole(c, mine)], send, recv, right)
        if kind == 8:
            return remote(full.at[xq, :, whole(c, mine)], full.at[xq, :, whole(c, mine)], send, recv, left)
        if kind == 9:
            return remote(full.at[x_before, :, plus(c, mine)], full.at[x_before, :, plus(c, mine)], send, recv, right)
        if kind == 10:
            return remote(full.at[x_after, :, minus(c, mine)], full.at[x_after, :, minus(c, mine)], send, recv, left)
        return remote(full.at[:, :, whole(c, mine)], full.at[:, :, whole(c, mine)], send, recv, partner)

    def stat_arrival(kind, c, mine):
        send, recv = ss_sem.at[kind, c], sr_sem.at[kind, c]
        if kind < 6:
            dst = landing(kind, c, mine)
        elif kind == 6:
            dst = halves.at[:, :, pl.ds(c * half, half)] if mine else across.at[:, pl.ds((c - FIRST) * chunk, chunk)]
        elif kind == 7:
            dst = full.at[x_before, :, whole(c, mine)]
        elif kind == 8:
            dst = full.at[x_after, :, whole(c, mine)]
        elif kind == 9:
            dst = full.at[x_far, :, plus(c, mine)]
        elif kind == 10:
            dst = full.at[x_far, :, minus(c, mine)]
        else:
            dst = full.at[:, :, other(c)]
        return remote(dst, dst, send, recv, partner)

    def begin(c, mine):
        u_store(c).start()
        if mine:
            stat(6, c, mine).start()
        else:
            for kind in range(4):
                stat(kind, c, mine).start()

    def join_halves(c, mine):
        stat_arrival(6, c, mine).wait_recv()
        span, there = whole(c, mine), pl.ds(c * half, half)
        for g in range(groups):
            total, square = merge(part[g, 0, span], part[g, 1, span], 4.0, halves[g, 0, there], halves[g, 1, there], 4.0)
            part[g, 0, span] = total
            part[g, 1, span] = square
        for kind in range(4):
            stat(kind, c, mine).start()

    def arrived(kind, c, mine):
        if mine:
            return ring[kind, 0, c, pl.ds(0, half // 2)], ring[kind, 1, c, pl.ds(0, half // 2)]
        return ring[kind, 0, c], ring[kind, 1, c]

    def hand_on_sums(c, mine):
        one = 8.0 if mine else 4.0
        for kind, owner, span in ((0, x_after, plus(c, mine)), (1, x_before, minus(c, mine))):
            stat_arrival(kind, c, mine).wait_recv()
            total, square = merge(part[owner, 0, span], part[owner, 1, span], one, *arrived(kind, c, mine), one)
            part[owner, 0, span] = total
            part[owner, 1, span] = square
            stat(4 + kind, c, mine).start()

    def finish(total, square, span):
        full[xq, 0, span] = total * (1.0 / 32.0)
        full[xq, 1, span] = lax.rsqrt(square * (1.0 / 32.0) + 0.0001)

    def own_sums(c, mine):
        one = 8.0 if mine else 4.0
        for kind in (2, 3, 4, 5):
            stat_arrival(kind, c, mine).wait_recv()
        for near, far, span in ((3, 4, plus(c, mine)), (2, 5, minus(c, mine))):
            total, square = merge(part[xq, 0, span], part[xq, 1, span], one, *arrived(near, c, mine), one)
            total, square = merge(total, square, 2 * one, *arrived(far, c, mine), 2 * one)
            if mine:
                finish(total, square, span)
            else:
                part[xq, 0, span] = total
                part[xq, 1, span] = square
        if mine:
            stat(7, c, mine).start()
            stat(8, c, mine).start()
        else:
            stat(6, c, mine).start()

    def join_partner(c, mine):
        stat_arrival(6, c, mine).wait_recv()
        for offset in (0, half):
            span, there = pl.ds(c * chunk + offset, half), pl.ds((c - FIRST) * chunk + offset, half)
            finish(*merge(part[xq, 0, span], part[xq, 1, span], 16.0, across[0, there], across[1, there], 16.0), span)
        stat(7, c, mine).start()
        stat(8, c, mine).start()

    def hand_on_results(c, mine):
        stat_arrival(7, c, mine).wait_recv()
        stat(9, c, mine).start()
        stat_arrival(8, c, mine).wait_recv()
        stat(10, c, mine).start()

    def collect(c, mine):
        stat_arrival(9, c, mine).wait_recv()
        stat_arrival(10, c, mine).wait_recv()
        if mine:
            stat(11, c, mine).start()
        else:
            f_store(c).start()

    def last_half(c, mine):
        stat_arrival(11, c, mine).wait_recv()
        f_store(c).start()

    rounds = {
        True: (begin, join_halves, hand_on_sums, own_sums, hand_on_results, collect, last_half),
        False: (begin, hand_on_sums, own_sums, join_partner, hand_on_results, collect),
    }
    bounds = {True: (0, FIRST), False: (FIRST, NC)}

    @pl.loop(0, NC + 6)
    def _(k):
        @pl.when(k < NC)
        def _():
            compute(STEPS - 1, k)

        for delay in range(7):
            for mine in (True, False):
                low, high = bounds[mine]
                if delay < len(rounds[mine]) and low < high:
                    @pl.when(jnp.logical_and(k >= low + delay, k < high + delay))
                    def _():
                        rounds[mine][delay](k - delay, mine)

    @pl.loop(0, NC)
    def _(c):
        for side in range(2):
            @pl.when(has["x", side])
            def _():
                x_copy((STEPS - 1) % 2, c, side).wait_send()

            @pl.when(has["z", side])
            def _():
                z_copy((STEPS - 1) % 2, c, side).wait_send()

        for side in range(2):
            @pl.when(jnp.logical_and(carries[side], odd(c)))
            def _():
                for step in range(STEPS):
                    pass_on(step, c, side).wait_send()

        for mine in (True, False):
            low, high = bounds[mine]

            @pl.when(jnp.logical_and(c >= low, c < high))
            def _():
                for kind in range(12 if mine else 11):
                    stat(kind, c, mine).wait_send()

        u_store(c).wait()
        f_store(c).wait()

    for side in range(2):
        @pl.when(has["y", side])
        def _():
            y_copy((STEPS - 1) % 2, side).wait_send()


def finish_kernel(u_ref, f_ref, norm_ref, end_ref):
    value = u_ref[...]
    end_ref[...] = value
    for g in range(4):
        band = slice(8 * g, 8 * g + 8)
        norm_ref[:, :, band] = (value[:, :, band] - f_ref[g, 0][:, None]) * f_ref[g, 1][:, None]


def body(u, k, q):
    rows, cols, height, lanes = u.shape
    dma = pltpu.SemaphoreType.DMA
    moved, stats = pl.pallas_call(
        main_kernel,
        out_shape=(
            jax.ShapeDtypeStruct(u.shape, F32),
            jax.ShapeDtypeStruct((4, 2, rows, 8, lanes), F32),
        ),
        in_specs=[pl.BlockSpec(memory_space=pl.ANY)] * 3,
        out_specs=[pl.BlockSpec(memory_space=pl.ANY)] * 2,
        scratch_shapes=[
            pltpu.VMEM((2, rows + 2, cols + 2, height, lanes), F32),
            pltpu.VMEM(u.shape, F32),
            pltpu.VMEM(u.shape, F32),
            pltpu.VMEM((2, 2, rows, cols, lanes), F32),
            pltpu.VMEM((2, 2, rows, cols, lanes), F32),
            pltpu.VMEM((4, 2, rows, 8, lanes), F32),
            pltpu.VMEM((4, 2, rows, 8, lanes), F32),
            pltpu.VMEM((6, 2, NC, rows // NC // 2, 8, lanes), F32),
            pltpu.VMEM((2, max(NC - FIRST, 1) * (rows // NC), 8, lanes), F32),
            pltpu.VMEM((4, 2, max(FIRST, 1) * (rows // NC // 2), 8, lanes), F32),
            pltpu.VMEM((STEPS, NC // 2, rows // NC, height, lanes), F32),
            dma((3, NC)), dma((2, NC)), dma((STEPS, NC // 2)), dma((STEPS, NC // 2)),
            dma((2, 2, NC)), dma((2, 2, NC)), dma((2, 2, NC)), dma((2, 2, NC)),
            dma((2, 2)), dma((2, 2)), dma((12, NC)), dma((12, NC)),
        ],
        compiler_params=pltpu.CompilerParams(
            collective_id=0, has_side_effects=True, vmem_limit_bytes=63 * 1024 * 1024
        ),
        name="heat_steps",
    )(u, k, q)
    tile = 32
    block = pl.BlockSpec((tile, cols, height, lanes), lambda i: (i, 0, 0, 0))
    return pl.pallas_call(
        finish_kernel,
        grid=(rows // tile,),
        out_shape=(jax.ShapeDtypeStruct(u.shape, F32),) * 2,
        in_specs=[block, pl.BlockSpec((4, 2, tile, 8, lanes), lambda i: (0, 0, i, 0, 0))],
        out_specs=[block, block],
        name="centre_and_scale",
    )(moved, stats)


def solution(mesh):
    placed = P("py", "px", "pz", None)
    return jax.shard_map(
        body, mesh=mesh, in_specs=(placed, placed, placed), out_specs=(placed, placed), check_vma=False
    )
```

```python
import jax
import jax.numpy as jnp
from jax import lax
from jax.experimental import pallas as pl
from jax.experimental.pallas import tpu as pltpu
from jax.sharding import PartitionSpec as P

STEPS = 4
NC = 8
LEAD = 3
FIRST = 5
MESH = pl.DeviceIdType.MESH
F32 = jnp.float32


def merge(sum_a, square_a, count_a, sum_b, square_b, count_b):
    gap = sum_a * (1.0 / count_a) - sum_b * (1.0 / count_b)
    weight = count_a * count_b / (count_a + count_b)
    return sum_a + sum_b, square_a + square_b + gap * gap * weight


def main_kernel(
    u_in, k_in, q_in, cond, full,
    field, supply, zsend, zrecv, part, ring, across, halves, passing,
    load_sem, ps_sem, pr_sem, xs_sem, xr_sem, zs_sem, zr_sem, ys_sem, yr_sem, ss_sem, sr_sem,
):
    rows, cols, height, lanes = u_in.shape
    chunk = rows // NC
    half = chunk // 2
    py, px, pz = lax.axis_index("py"), lax.axis_index("px"), lax.axis_index("pz")
    ny, nx, nz = lax.axis_size("py"), lax.axis_size("px"), lax.axis_size("pz")
    groups = 4
    xq = lax.rem(px, groups)
    zq = px - xq
    right = {"px": zq + lax.rem(xq + 1, groups)}
    left = {"px": zq + lax.rem(xq + groups - 1, groups)}
    partner = {"px": lax.rem(px + groups, nx)}
    x_after, x_before = lax.rem(xq + 1, groups), lax.rem(xq + groups - 1, groups)
    x_far = lax.rem(xq + 2, groups)

    has = {
        ("x", 0): px > 0, ("x", 1): px < nx - 1,
        ("y", 0): py > 0, ("y", 1): py < ny - 1,
        ("z", 0): pz > 0, ("z", 1): pz < nz - 1,
    }
    peer = {
        ("x", 0): {"px": px - 1}, ("x", 1): {"px": px + 1},
        ("y", 0): {"py": py - 1}, ("y", 1): {"py": py + 1},
        ("z", 0): {"pz": pz - 1}, ("z", 1): {"pz": pz + 1},
    }

    barrier = pltpu.get_barrier_semaphore()
    count = jnp.int32(3)
    for key in has:
        count = count + has[key].astype(jnp.int32)

        @pl.when(has[key])
        def _():
            pl.semaphore_signal(barrier, inc=1, device_id=peer[key], device_id_type=MESH)

    for other in (right, left, partner):
        pl.semaphore_signal(barrier, inc=1, device_id=other, device_id_type=MESH)

    def load(c, which):
        span = pl.ds(c * chunk, chunk)
        if which == 0:
            return pltpu.make_async_copy(
                u_in.at[span], field.at[0, pl.ds(c * chunk + 1, chunk), pl.ds(1, cols)], load_sem.at[0, c]
            )
        source, target = ((k_in, cond), (q_in, supply))[which - 1]
        return pltpu.make_async_copy(source.at[span], target.at[span], load_sem.at[which, c])

    def remote(src, dst, send, recv, device):
        return pltpu.make_async_remote_copy(
            src_ref=src, dst_ref=dst, send_sem=send, recv_sem=recv, device_id=device, device_id_type=MESH
        )

    def x_copy(slot, c, side, first=False):
        span = pl.ds(c * chunk, chunk)
        padded = pl.ds(c * chunk + 1, chunk)
        edge = 0 if side == 0 else cols - 1
        src = u_in.at[span, edge] if first else field.at[slot, padded, edge + 1]
        return remote(
            src, field.at[slot, padded, cols + 1 if side == 0 else 0],
            xs_sem.at[side, slot, c], xr_sem.at[1 - side, slot, c], peer["x", side],
        )

    middle = nx // 2
    at_seam = (px == middle, px == middle - 1)
    carries = (px == 0, px == nx - 1)

    def odd(c):
        return lax.rem(c, 2) == 1

    def x_detour(slot, c, side, step):
        edge = 0 if side == 0 else cols - 1
        if step == 0:
            src = u_in.at[pl.ds(c * chunk, chunk), edge]
        else:
            src = field.at[slot, pl.ds(c * chunk + 1, chunk), edge + 1]
        return remote(
            src, passing.at[step, lax.div(c, 2)],
            xs_sem.at[side, slot, c], pr_sem.at[step, lax.div(c, 2)], partner,
        )

    def x_start(step, c, side):
        slot = step % 2
        detour = jnp.logical_and(at_seam[side], odd(c))

        @pl.when(detour)
        def _():
            x_detour(slot, c, side, step).start()

        @pl.when(jnp.logical_not(detour))
        def _():
            x_copy(slot, c, side, step == 0).start()

    def pass_on(step, c, side):
        here, slot = passing.at[step, lax.div(c, 2)], step % 2
        return remote(
            here, field.at[slot, pl.ds(c * chunk + 1, chunk), cols + 1 if side == 0 else 0],
            ps_sem.at[step, lax.div(c, 2)], xr_sem.at[1 - side, slot, c],
            {"px": middle - 1 if side == 0 else middle},
        )

    def relay(step, c):
        here = passing.at[step, lax.div(c, 2)]
        for side in range(2):
            @pl.when(jnp.logical_and(carries[side], odd(c)))
            def _():
                remote(
                    here, here, ps_sem.at[step, lax.div(c, 2)], pr_sem.at[step, lax.div(c, 2)], partner
                ).wait_recv()
                pass_on(step, c, side).start()

    def x_arrival(slot, c, side):
        padded = pl.ds(c * chunk + 1, chunk)
        dst = field.at[slot, padded, 0 if side == 0 else cols + 1]
        return remote(dst, dst, xs_sem.at[side, slot, c], xr_sem.at[side, slot, c], peer["x", side])

    def z_copy(slot, c, side):
        span = pl.ds(c * chunk, chunk)
        return remote(
            zsend.at[slot, side, span], zrecv.at[slot, 1 - side, span],
            zs_sem.at[side, slot, c], zr_sem.at[1 - side, slot, c], peer["z", side],
        )

    def z_arrival(slot, c, side):
        dst = zrecv.at[slot, side, pl.ds(c * chunk, chunk)]
        return remote(dst, dst, zs_sem.at[side, slot, c], zr_sem.at[side, slot, c], peer["z", side])

    def y_copy(slot, side, first=False):
        inner = pl.ds(1, cols)
        row = 0 if side == 0 else rows - 1
        src = u_in.at[row] if first else field.at[slot, row + 1, inner]
        return remote(
            src, field.at[slot, rows + 1 if side == 0 else 0, inner],
            ys_sem.at[side, slot], yr_sem.at[1 - side, slot], peer["y", side],
        )

    def y_arrival(slot, side):
        dst = field.at[slot, 0 if side == 0 else rows + 1, pl.ds(1, cols)]
        return remote(dst, dst, ys_sem.at[side, slot], yr_sem.at[side, slot], peer["y", side])

    for which in range(3):
        @pl.loop(0, NC)
        def _(c):
            load(c, which).start()

    pl.semaphore_wait(barrier, count)

    for side in range(2):
        @pl.when(has["x", side])
        def _():
            @pl.loop(0, LEAD)
            def _(c):
                x_start(0, c, side)

        @pl.when(has["y", side])
        def _():
            y_copy(0, side, first=True).start()

    zero_column = jnp.zeros((height, lanes), F32)
    zero_edge = jnp.zeros((cols, lanes), F32)
    for side in range(2):
        @pl.when(jnp.logical_not(has["x", side]))
        def _():
            @pl.loop(0, rows)
            def _(y):
                for slot in range(2):
                    field[slot, y + 1, 0 if side == 0 else cols + 1] = zero_column

        @pl.when(jnp.logical_not(has["y", side]))
        def _():
            for slot in range(2):
                for x in range(cols):
                    field[slot, 0 if side == 0 else rows + 1, x + 1] = zero_column

        @pl.when(jnp.logical_not(has["z", side]))
        def _():
            @pl.loop(0, rows)
            def _(y):
                for slot in range(2):
                    zrecv[slot, side, y] = zero_edge

    def pack(slot, y, x, value):
        zsend[slot, 0, y, x : x + 1] = value[0:1]
        zsend[slot, 1, y, x : x + 1] = value[height - 1 : height]

    @pl.loop(0, NC)
    def _(c):
        load(c, 0).wait()

        @pl.loop(0, chunk)
        def _(r):
            y = c * chunk + r
            for x in range(cols):
                pack(0, y, x, field[0, y + 1, x + 1])

        for side in range(2):
            @pl.when(has["z", side])
            def _():
                z_copy(0, c, side).start()

    row_index = lax.broadcasted_iota(jnp.int32, (height, lanes), 0)
    at_low, at_high = row_index == 0, row_index == height - 1

    def send_faces(step, c):
        for side in range(2):
            @pl.when(has["x", side])
            def _():
                x_start(step, c, side)

    def compute(step, c):
        src, dst = step % 2, (step + 1) % 2
        if step == 0:
            load(c, 1).wait()
            load(c, 2).wait()

            @pl.when(c < LEAD - 1)
            def _():
                relay(0, c)

        for side in range(2):
            @pl.when(has["x", side])
            def _():
                x_arrival(src, c, side).wait_recv()
                if step >= 1:
                    x_copy(dst, c, side).wait_send()

            @pl.when(has["z", side])
            def _():
                z_arrival(src, c, side).wait_recv()
                if step >= 1:
                    z_copy(dst, c, side).wait_send()

            @pl.when(jnp.logical_and(has["y", side], c == (0 if side == 0 else NC - 1)))
            def _():
                y_arrival(src, side).wait_recv()
                if step >= 1:
                    y_copy(dst, side).wait_send()

        @pl.loop(0, chunk)
        def _(r):
            y = c * chunk + r
            fresh = []
            for x in range(cols):
                here = field[src, y + 1, x + 1]
                below = jnp.where(at_low, zrecv[src, 0, y, x : x + 1], pltpu.roll(here, 1, 0))
                above = jnp.where(at_high, zrecv[src, 1, y, x : x + 1], pltpu.roll(here, height - 1, 0))
                spread = (
                    field[src, y, x + 1] + field[src, y + 2, x + 1]
                    + field[src, y + 1, x] + field[src, y + 1, x + 2]
                    + below + above - 6.0 * here
                )
                value = here + cond[y, x] * spread + supply[y, x]
                if step < STEPS - 1:
                    field[dst, y + 1, x + 1] = value
                    pack(dst, y, x, value)
                else:
                    cond[y, x] = value
                fresh.append(value)
            if step == STEPS - 1:
                total = (fresh[0] + fresh[1]) + (fresh[2] + fresh[3])
                middle = total * (1.0 / cols)
                square = None
                for value in fresh:
                    away = value - middle
                    square = away * away if square is None else square + away * away
                for g in range(groups):
                    part[g, 0, y] = total[8 * g : 8 * g + 8]
                    part[g, 1, y] = square[8 * g : 8 * g + 8]

        if step < STEPS - 1:
            for side in range(2):
                @pl.when(has["z", side])
                def _():
                    z_copy(dst, c, side).start()

                @pl.when(jnp.logical_and(has["y", side], c == (0 if side == 0 else NC - 1)))
                def _():
                    y_copy(dst, side).start()

        for ahead, act in ((LEAD, send_faces), (LEAD - 1, relay)):
            @pl.when(c < NC - ahead)
            def _():
                act(step, c + ahead)

            if step < STEPS - 1:
                @pl.when(c >= NC - ahead)
                def _():
                    act(step + 1, c + ahead - NC)

    for step in range(STEPS - 1):
        @pl.loop(0, NC)
        def _(c):
            compute(step, c)

    lower = lax.div(px, groups)

    def span_of(c, mine):
        if mine:
            return c * chunk + lower * half, half // 2
        return c * chunk, half

    def plus(c, mine):
        start, size = span_of(c, mine)
        return pl.ds(start, size)

    def minus(c, mine):
        start, size = span_of(c, mine)
        return pl.ds(start + size, size)

    def whole(c, mine):
        start, size = span_of(c, mine)
        return pl.ds(start, 2 * size)

    def other(c):
        return pl.ds(c * chunk + (1 - lower) * half, half)

    def landing(kind, c, mine):
        return ring.at[kind, :, c, pl.ds(0, half // 2)] if mine else ring.at[kind, :, c]

    def stat(kind, c, mine):
        send, recv = ss_sem.at[kind, c], sr_sem.at[kind, c]
        if kind == 0:
            return remote(part.at[x_far, :, plus(c, mine)], landing(0, c, mine), send, recv, right)
        if kind == 1:
            return remote(part.at[x_far, :, minus(c, mine)], landing(1, c, mine), send, recv, left)
        if kind == 2:
            return remote(part.at[x_after, :, minus(c, mine)], landing(2, c, mine), send, recv, right)
        if kind == 3:
            return remote(part.at[x_before, :, plus(c, mine)], landing(3, c, mine), send, recv, left)
        if kind == 4:
            return remote(part.at[x_after, :, plus(c, mine)], landing(4, c, mine), send, recv, right)
        if kind == 5:
            return remote(part.at[x_before, :, minus(c, mine)], landing(5, c, mine), send, recv, left)
        if kind == 6:
            if mine:
                return remote(part.at[:, :, other(c)], halves.at[:, :, pl.ds(c * half, half)], send, recv, partner)
            return remote(part.at[xq, :, whole(c, mine)], across.at[:, pl.ds((c - FIRST) * chunk, chunk)], send, recv, partner)
        if kind == 7:
            return remote(full.at[xq, :, whole(c, mine)], full.at[xq, :, whole(c, mine)], send, recv, right)
        if kind == 8:
            return remote(full.at[xq, :, whole(c, mine)], full.at[xq, :, whole(c, mine)], send, recv, left)
        if kind == 9:
            return remote(full.at[x_before, :, plus(c, mine)], full.at[x_before, :, plus(c, mine)], send, recv, right)
        if kind == 10:
            return remote(full.at[x_after, :, minus(c, mine)], full.at[x_after, :, minus(c, mine)], send, recv, left)
        return remote(full.at[:, :, whole(c, mine)], full.at[:, :, whole(c, mine)], send, recv, partner)

    def stat_arrival(kind, c, mine):
        send, recv = ss_sem.at[kind, c], sr_sem.at[kind, c]
        if kind < 6:
            dst = landing(kind, c, mine)
        elif kind == 6:
            dst = halves.at[:, :, pl.ds(c * half, half)] if mine else across.at[:, pl.ds((c - FIRST) * chunk, chunk)]
        elif kind == 7:
            dst = full.at[x_before, :, whole(c, mine)]
        elif kind == 8:
            dst = full.at[x_after, :, whole(c, mine)]
        elif kind == 9:
            dst = full.at[x_far, :, plus(c, mine)]
        elif kind == 10:
            dst = full.at[x_far, :, minus(c, mine)]
        else:
            dst = full.at[:, :, other(c)]
        return remote(dst, dst, send, recv, partner)

    def begin(c, mine):
        if mine:
            stat(6, c, mine).start()
        else:
            for kind in range(4):
                stat(kind, c, mine).start()

    def join_halves(c, mine):
        stat_arrival(6, c, mine).wait_recv()
        span, there = whole(c, mine), pl.ds(c * half, half)
        for g in range(groups):
            total, square = merge(part[g, 0, span], part[g, 1, span], 4.0, halves[g, 0, there], halves[g, 1, there], 4.0)
            part[g, 0, span] = total
            part[g, 1, span] = square
        for kind in range(4):
            stat(kind, c, mine).start()

    def arrived(kind, c, mine):
        if mine:
            return ring[kind, 0, c, pl.ds(0, half // 2)], ring[kind, 1, c, pl.ds(0, half // 2)]
        return ring[kind, 0, c], ring[kind, 1, c]

    def hand_on_sums(c, mine):
        one = 8.0 if mine else 4.0
        for kind, owner, span in ((0, x_after, plus(c, mine)), (1, x_before, minus(c, mine))):
            stat_arrival(kind, c, mine).wait_recv()
            total, square = merge(part[owner, 0, span], part[owner, 1, span], one, *arrived(kind, c, mine), one)
            part[owner, 0, span] = total
            part[owner, 1, span] = square
            stat(4 + kind, c, mine).start()

    def finish(total, square, span):
        full[xq, 0, span] = total * (1.0 / 32.0)
        full[xq, 1, span] = lax.rsqrt(square * (1.0 / 32.0) + 0.0001)

    def own_sums(c, mine):
        one = 8.0 if mine else 4.0
        for kind in (2, 3, 4, 5):
            stat_arrival(kind, c, mine).wait_recv()
        for near, far, span in ((3, 4, plus(c, mine)), (2, 5, minus(c, mine))):
            total, square = merge(part[xq, 0, span], part[xq, 1, span], one, *arrived(near, c, mine), one)
            total, square = merge(total, square, 2 * one, *arrived(far, c, mine), 2 * one)
            if mine:
                finish(total, square, span)
            else:
                part[xq, 0, span] = total
                part[xq, 1, span] = square
        if mine:
            stat(7, c, mine).start()
            stat(8, c, mine).start()
        else:
            stat(6, c, mine).start()

    def join_partner(c, mine):
        stat_arrival(6, c, mine).wait_recv()
        for offset in (0, half):
            span, there = pl.ds(c * chunk + offset, half), pl.ds((c - FIRST) * chunk + offset, half)
            finish(*merge(part[xq, 0, span], part[xq, 1, span], 16.0, across[0, there], across[1, there], 16.0), span)
        stat(7, c, mine).start()
        stat(8, c, mine).start()

    def hand_on_results(c, mine):
        stat_arrival(7, c, mine).wait_recv()
        stat(9, c, mine).start()
        stat_arrival(8, c, mine).wait_recv()
        stat(10, c, mine).start()

    def collect(c, mine):
        stat_arrival(9, c, mine).wait_recv()
        stat_arrival(10, c, mine).wait_recv()
        if mine:
            stat(11, c, mine).start()

    def last_half(c, mine):
        stat_arrival(11, c, mine).wait_recv()

    rounds = {
        True: (begin, join_halves, hand_on_sums, own_sums, hand_on_results, collect, last_half),
        False: (begin, hand_on_sums, own_sums, join_partner, hand_on_results, collect),
    }
    bounds = {True: (0, FIRST), False: (FIRST, NC)}

    @pl.loop(0, NC + 6)
    def _(k):
        @pl.when(k < NC)
        def _():
            compute(STEPS - 1, k)

        for delay in range(7):
            for mine in (True, False):
                low, high = bounds[mine]
                if delay < len(rounds[mine]) and low < high:
                    @pl.when(jnp.logical_and(k >= low + delay, k < high + delay))
                    def _():
                        rounds[mine][delay](k - delay, mine)

    @pl.loop(0, NC)
    def _(c):
        for side in range(2):
            @pl.when(has["x", side])
            def _():
                x_copy((STEPS - 1) % 2, c, side).wait_send()

            @pl.when(has["z", side])
            def _():
                z_copy((STEPS - 1) % 2, c, side).wait_send()

        for side in range(2):
            @pl.when(jnp.logical_and(carries[side], odd(c)))
            def _():
                for step in range(STEPS):
                    pass_on(step, c, side).wait_send()

        for mine in (True, False):
            low, high = bounds[mine]

            @pl.when(jnp.logical_and(c >= low, c < high))
            def _():
                for kind in range(12 if mine else 11):
                    stat(kind, c, mine).wait_send()


    for side in range(2):
        @pl.when(has["y", side])
        def _():
            y_copy((STEPS - 1) % 2, side).wait_send()


def finish_kernel(u_ref, f_ref, norm_ref, end_ref, sem):
    step = pl.program_id(0)
    out = pltpu.make_async_copy(u_ref, end_ref, sem)

    @pl.when(step == 0)
    def _():
        out.start()

    tile = norm_ref.shape[0]

    @pl.loop(0, tile)
    def _(r):
        y = step * tile + r
        for x in range(u_ref.shape[1]):
            for g in range(4):
                band = slice(8 * g, 8 * g + 8)
                norm_ref[r, x, band] = (u_ref[y, x, band] - f_ref[g, 0, y]) * f_ref[g, 1, y]

    @pl.when(step == pl.num_programs(0) - 1)
    def _():
        out.wait()


def body(u, k, q):
    rows, cols, height, lanes = u.shape
    dma = pltpu.SemaphoreType.DMA
    moved, stats = pl.pallas_call(
        main_kernel,
        out_shape=(
            pltpu.VMEM(u.shape, F32),
            pltpu.VMEM((4, 2, rows, 8, lanes), F32),
        ),
        in_specs=[pl.BlockSpec(memory_space=pl.ANY)] * 3,
        out_specs=[pl.BlockSpec(memory_space=pltpu.VMEM)] * 2,
        scratch_shapes=[
            pltpu.VMEM((2, rows + 2, cols + 2, height, lanes), F32),
            pltpu.VMEM(u.shape, F32),
            pltpu.VMEM((2, 2, rows, cols, lanes), F32),
            pltpu.VMEM((2, 2, rows, cols, lanes), F32),
            pltpu.VMEM((4, 2, rows, 8, lanes), F32),
            pltpu.VMEM((6, 2, NC, rows // NC // 2, 8, lanes), F32),
            pltpu.VMEM((2, max(NC - FIRST, 1) * (rows // NC), 8, lanes), F32),
            pltpu.VMEM((4, 2, max(FIRST, 1) * (rows // NC // 2), 8, lanes), F32),
            pltpu.VMEM((STEPS, NC // 2, rows // NC, height, lanes), F32),
            dma((3, NC)), dma((STEPS, NC // 2)), dma((STEPS, NC // 2)),
            dma((2, 2, NC)), dma((2, 2, NC)), dma((2, 2, NC)), dma((2, 2, NC)),
            dma((2, 2)), dma((2, 2)), dma((12, NC)), dma((12, NC)),
        ],
        compiler_params=pltpu.CompilerParams(
            collective_id=0, has_side_effects=True, vmem_limit_bytes=49 * 1024 * 1024
        ),
        name="heat_steps",
    )(u, k, q)
    tile = 16
    return pl.pallas_call(
        finish_kernel,
        grid=(rows // tile,),
        out_shape=(jax.ShapeDtypeStruct(u.shape, F32),) * 2,
        in_specs=[pl.BlockSpec(memory_space=pltpu.VMEM)] * 2,
        out_specs=[
            pl.BlockSpec((tile, cols, height, lanes), lambda i: (i, 0, 0, 0)),
            pl.BlockSpec(memory_space=pl.ANY),
        ],
        scratch_shapes=[dma],
        compiler_params=pltpu.CompilerParams(vmem_limit_bytes=8 * 1024 * 1024),
        name="centre_and_scale",
    )(moved, stats)


def solution(mesh):
    placed = P("py", "px", "pz", None)
    return jax.shard_map(
        body, mesh=mesh, in_specs=(placed, placed, placed), out_specs=(placed, placed), check_vma=False
    )
```

```python
import jax
import jax.numpy as jnp
from jax import lax
from jax.experimental import pallas as pl
from jax.experimental.pallas import tpu as pltpu
from jax.sharding import PartitionSpec as P

STEPS = 4
NC = 8
LEAD = 3
FIRST = 6
MESH = pl.DeviceIdType.MESH
F32 = jnp.float32


def merge(sum_a, square_a, count_a, sum_b, square_b, count_b):
    gap = sum_a * (1.0 / count_a) - sum_b * (1.0 / count_b)
    weight = count_a * count_b / (count_a + count_b)
    return sum_a + sum_b, square_a + square_b + gap * gap * weight


def main_kernel(
    u_in, k_in, q_in, cond, full,
    field, supply, zsend, zrecv, part, ring, across, halves, passing,
    load_sem, ps_sem, pr_sem, xs_sem, xr_sem, zs_sem, zr_sem, ys_sem, yr_sem, ss_sem, sr_sem,
):
    rows, cols, height, lanes = u_in.shape
    chunk = rows // NC
    half = chunk // 2
    py, px, pz = lax.axis_index("py"), lax.axis_index("px"), lax.axis_index("pz")
    ny, nx, nz = lax.axis_size("py"), lax.axis_size("px"), lax.axis_size("pz")
    groups = 4
    xq = lax.rem(px, groups)
    zq = px - xq
    right = {"px": zq + lax.rem(xq + 1, groups)}
    left = {"px": zq + lax.rem(xq + groups - 1, groups)}
    partner = {"px": lax.rem(px + groups, nx)}
    x_after, x_before = lax.rem(xq + 1, groups), lax.rem(xq + groups - 1, groups)
    x_far = lax.rem(xq + 2, groups)

    has = {
        ("x", 0): px > 0, ("x", 1): px < nx - 1,
        ("y", 0): py > 0, ("y", 1): py < ny - 1,
        ("z", 0): pz > 0, ("z", 1): pz < nz - 1,
    }
    peer = {
        ("x", 0): {"px": px - 1}, ("x", 1): {"px": px + 1},
        ("y", 0): {"py": py - 1}, ("y", 1): {"py": py + 1},
        ("z", 0): {"pz": pz - 1}, ("z", 1): {"pz": pz + 1},
    }

    barrier = pltpu.get_barrier_semaphore()
    count = jnp.int32(3)
    for key in has:
        count = count + has[key].astype(jnp.int32)

        @pl.when(has[key])
        def _():
            pl.semaphore_signal(barrier, inc=1, device_id=peer[key], device_id_type=MESH)

    for other in (right, left, partner):
        pl.semaphore_signal(barrier, inc=1, device_id=other, device_id_type=MESH)

    def load(c, which):
        span = pl.ds(c * chunk, chunk)
        if which == 0:
            return pltpu.make_async_copy(
                u_in.at[span], field.at[0, pl.ds(c * chunk + 1, chunk), pl.ds(1, cols)], load_sem.at[0, c]
            )
        source, target = ((k_in, cond), (q_in, supply))[which - 1]
        return pltpu.make_async_copy(source.at[span], target.at[span], load_sem.at[which, c])

    def remote(src, dst, send, recv, device):
        return pltpu.make_async_remote_copy(
            src_ref=src, dst_ref=dst, send_sem=send, recv_sem=recv, device_id=device, device_id_type=MESH
        )

    def x_copy(slot, c, side, first=False):
        span = pl.ds(c * chunk, chunk)
        padded = pl.ds(c * chunk + 1, chunk)
        edge = 0 if side == 0 else cols - 1
        src = u_in.at[span, edge] if first else field.at[slot, padded, edge + 1]
        return remote(
            src, field.at[slot, padded, cols + 1 if side == 0 else 0],
            xs_sem.at[side, slot, c], xr_sem.at[1 - side, slot, c], peer["x", side],
        )

    middle = nx // 2
    at_seam = (px == middle, px == middle - 1)
    carries = (px == 0, px == nx - 1)

    def odd(c):
        return lax.rem(c, 2) == 1

    def x_detour(slot, c, side, step):
        edge = 0 if side == 0 else cols - 1
        if step == 0:
            src = u_in.at[pl.ds(c * chunk, chunk), edge]
        else:
            src = field.at[slot, pl.ds(c * chunk + 1, chunk), edge + 1]
        return remote(
            src, passing.at[step, lax.div(c, 2)],
            xs_sem.at[side, slot, c], pr_sem.at[step, lax.div(c, 2)], partner,
        )

    def x_start(step, c, side):
        slot = step % 2
        detour = jnp.logical_and(at_seam[side], odd(c))

        @pl.when(detour)
        def _():
            x_detour(slot, c, side, step).start()

        @pl.when(jnp.logical_not(detour))
        def _():
            x_copy(slot, c, side, step == 0).start()

    def pass_on(step, c, side):
        here, slot = passing.at[step, lax.div(c, 2)], step % 2
        return remote(
            here, field.at[slot, pl.ds(c * chunk + 1, chunk), cols + 1 if side == 0 else 0],
            ps_sem.at[step, lax.div(c, 2)], xr_sem.at[1 - side, slot, c],
            {"px": middle - 1 if side == 0 else middle},
        )

    def relay(step, c):
        here = passing.at[step, lax.div(c, 2)]
        for side in range(2):
            @pl.when(jnp.logical_and(carries[side], odd(c)))
            def _():
                remote(
                    here, here, ps_sem.at[step, lax.div(c, 2)], pr_sem.at[step, lax.div(c, 2)], partner
                ).wait_recv()
                pass_on(step, c, side).start()

    def x_arrival(slot, c, side):
        padded = pl.ds(c * chunk + 1, chunk)
        dst = field.at[slot, padded, 0 if side == 0 else cols + 1]
        return remote(dst, dst, xs_sem.at[side, slot, c], xr_sem.at[side, slot, c], peer["x", side])

    def z_copy(slot, c, side):
        span = pl.ds(c * chunk, chunk)
        return remote(
            zsend.at[slot, side, span], zrecv.at[slot, 1 - side, span],
            zs_sem.at[side, slot, c], zr_sem.at[1 - side, slot, c], peer["z", side],
        )

    def z_arrival(slot, c, side):
        dst = zrecv.at[slot, side, pl.ds(c * chunk, chunk)]
        return remote(dst, dst, zs_sem.at[side, slot, c], zr_sem.at[side, slot, c], peer["z", side])

    def y_copy(slot, side, first=False):
        inner = pl.ds(1, cols)
        row = 0 if side == 0 else rows - 1
        src = u_in.at[row] if first else field.at[slot, row + 1, inner]
        return remote(
            src, field.at[slot, rows + 1 if side == 0 else 0, inner],
            ys_sem.at[side, slot], yr_sem.at[1 - side, slot], peer["y", side],
        )

    def y_arrival(slot, side):
        dst = field.at[slot, 0 if side == 0 else rows + 1, pl.ds(1, cols)]
        return remote(dst, dst, ys_sem.at[side, slot], yr_sem.at[side, slot], peer["y", side])

    for which in range(3):
        @pl.loop(0, NC)
        def _(c):
            load(c, which).start()

    pl.semaphore_wait(barrier, count)

    for side in range(2):
        @pl.when(has["x", side])
        def _():
            @pl.loop(0, LEAD)
            def _(c):
                x_start(0, c, side)

        @pl.when(has["y", side])
        def _():
            y_copy(0, side, first=True).start()

    zero_column = jnp.zeros((height, lanes), F32)
    zero_edge = jnp.zeros((cols, lanes), F32)
    for side in range(2):
        @pl.when(jnp.logical_not(has["x", side]))
        def _():
            @pl.loop(0, rows)
            def _(y):
                for slot in range(2):
                    field[slot, y + 1, 0 if side == 0 else cols + 1] = zero_column

        @pl.when(jnp.logical_not(has["y", side]))
        def _():
            for slot in range(2):
                for x in range(cols):
                    field[slot, 0 if side == 0 else rows + 1, x + 1] = zero_column

        @pl.when(jnp.logical_not(has["z", side]))
        def _():
            @pl.loop(0, rows)
            def _(y):
                for slot in range(2):
                    zrecv[slot, side, y] = zero_edge

    def pack(slot, y, x, value):
        zsend[slot, 0, y, x : x + 1] = value[0:1]
        zsend[slot, 1, y, x : x + 1] = value[height - 1 : height]

    @pl.loop(0, NC)
    def _(c):
        load(c, 0).wait()

        @pl.loop(0, chunk)
        def _(r):
            y = c * chunk + r
            for x in range(cols):
                pack(0, y, x, field[0, y + 1, x + 1])

        for side in range(2):
            @pl.when(has["z", side])
            def _():
                z_copy(0, c, side).start()

    row_index = lax.broadcasted_iota(jnp.int32, (height, lanes), 0)
    at_low, at_high = row_index == 0, row_index == height - 1

    def send_faces(step, c):
        for side in range(2):
            @pl.when(has["x", side])
            def _():
                x_start(step, c, side)

    def compute(step, c):
        src, dst = step % 2, (step + 1) % 2
        if step == 0:
            load(c, 1).wait()
            load(c, 2).wait()

            @pl.when(c < LEAD - 1)
            def _():
                relay(0, c)

        for side in range(2):
            @pl.when(has["x", side])
            def _():
                x_arrival(src, c, side).wait_recv()
                if step >= 1:
                    x_copy(dst, c, side).wait_send()

            @pl.when(has["z", side])
            def _():
                z_arrival(src, c, side).wait_recv()
                if step >= 1:
                    z_copy(dst, c, side).wait_send()

            @pl.when(jnp.logical_and(has["y", side], c == (0 if side == 0 else NC - 1)))
            def _():
                y_arrival(src, side).wait_recv()
                if step >= 1:
                    y_copy(dst, side).wait_send()

        @pl.loop(0, chunk)
        def _(r):
            y = c * chunk + r
            fresh = []
            for x in range(cols):
                here = field[src, y + 1, x + 1]
                below = jnp.where(at_low, zrecv[src, 0, y, x : x + 1], pltpu.roll(here, 1, 0))
                above = jnp.where(at_high, zrecv[src, 1, y, x : x + 1], pltpu.roll(here, height - 1, 0))
                spread = (
                    field[src, y, x + 1] + field[src, y + 2, x + 1]
                    + field[src, y + 1, x] + field[src, y + 1, x + 2]
                    + below + above - 6.0 * here
                )
                value = here + cond[y, x] * spread + supply[y, x]
                if step < STEPS - 1:
                    field[dst, y + 1, x + 1] = value
                    pack(dst, y, x, value)
                else:
                    cond[y, x] = value
                fresh.append(value)
            if step == STEPS - 1:
                total = (fresh[0] + fresh[1]) + (fresh[2] + fresh[3])
                middle = total * (1.0 / cols)
                square = None
                for value in fresh:
                    away = value - middle
                    square = away * away if square is None else square + away * away
                for g in range(groups):
                    part[g, 0, y] = total[8 * g : 8 * g + 8]
                    part[g, 1, y] = square[8 * g : 8 * g + 8]

        if step < STEPS - 1:
            for side in range(2):
                @pl.when(has["z", side])
                def _():
                    z_copy(dst, c, side).start()

                @pl.when(jnp.logical_and(has["y", side], c == (0 if side == 0 else NC - 1)))
                def _():
                    y_copy(dst, side).start()

        for ahead, act in ((LEAD, send_faces), (LEAD - 1, relay)):
            @pl.when(c < NC - ahead)
            def _():
                act(step, c + ahead)

            if step < STEPS - 1:
                @pl.when(c >= NC - ahead)
                def _():
                    act(step + 1, c + ahead - NC)

    for step in range(STEPS - 1):
        @pl.loop(0, NC)
        def _(c):
            compute(step, c)

    lower = lax.div(px, groups)

    def span_of(c, mine):
        if mine:
            return c * chunk + lower * half, half // 2
        return c * chunk, half

    def plus(c, mine):
        start, size = span_of(c, mine)
        return pl.ds(start, size)

    def minus(c, mine):
        start, size = span_of(c, mine)
        return pl.ds(start + size, size)

    def whole(c, mine):
        start, size = span_of(c, mine)
        return pl.ds(start, 2 * size)

    def other(c):
        return pl.ds(c * chunk + (1 - lower) * half, half)

    def landing(kind, c, mine):
        return ring.at[kind, :, c, pl.ds(0, half // 2)] if mine else ring.at[kind, :, c]

    def stat(kind, c, mine):
        send, recv = ss_sem.at[kind, c], sr_sem.at[kind, c]
        if kind == 0:
            return remote(part.at[x_far, :, plus(c, mine)], landing(0, c, mine), send, recv, right)
        if kind == 1:
            return remote(part.at[x_far, :, minus(c, mine)], landing(1, c, mine), send, recv, left)
        if kind == 2:
            return remote(part.at[x_after, :, minus(c, mine)], landing(2, c, mine), send, recv, right)
        if kind == 3:
            return remote(part.at[x_before, :, plus(c, mine)], landing(3, c, mine), send, recv, left)
        if kind == 4:
            return remote(part.at[x_after, :, plus(c, mine)], landing(4, c, mine), send, recv, right)
        if kind == 5:
            return remote(part.at[x_before, :, minus(c, mine)], landing(5, c, mine), send, recv, left)
        if kind == 6:
            if mine:
                return remote(part.at[:, :, other(c)], halves.at[:, :, pl.ds(c * half, half)], send, recv, partner)
            return remote(part.at[xq, :, whole(c, mine)], across.at[:, pl.ds((c - FIRST) * chunk, chunk)], send, recv, partner)
        if kind == 7:
            return remote(full.at[xq, :, whole(c, mine)], full.at[xq, :, whole(c, mine)], send, recv, right)
        if kind == 8:
            return remote(full.at[xq, :, whole(c, mine)], full.at[xq, :, whole(c, mine)], send, recv, left)
        if kind == 9:
            return remote(full.at[x_before, :, plus(c, mine)], full.at[x_before, :, plus(c, mine)], send, recv, right)
        if kind == 10:
            return remote(full.at[x_after, :, minus(c, mine)], full.at[x_after, :, minus(c, mine)], send, recv, left)
        return remote(full.at[:, :, whole(c, mine)], full.at[:, :, whole(c, mine)], send, recv, partner)

    def stat_arrival(kind, c, mine):
        send, recv = ss_sem.at[kind, c], sr_sem.at[kind, c]
        if kind < 6:
            dst = landing(kind, c, mine)
        elif kind == 6:
            dst = halves.at[:, :, pl.ds(c * half, half)] if mine else across.at[:, pl.ds((c - FIRST) * chunk, chunk)]
        elif kind == 7:
            dst = full.at[x_before, :, whole(c, mine)]
        elif kind == 8:
            dst = full.at[x_after, :, whole(c, mine)]
        elif kind == 9:
            dst = full.at[x_far, :, plus(c, mine)]
        elif kind == 10:
            dst = full.at[x_far, :, minus(c, mine)]
        else:
            dst = full.at[:, :, other(c)]
        return remote(dst, dst, send, recv, partner)

    def begin(c, mine):
        if mine:
            stat(6, c, mine).start()
        else:
            for kind in range(4):
                stat(kind, c, mine).start()

    def join_halves(c, mine):
        stat_arrival(6, c, mine).wait_recv()
        span, there = whole(c, mine), pl.ds(c * half, half)
        for g in range(groups):
            total, square = merge(part[g, 0, span], part[g, 1, span], 4.0, halves[g, 0, there], halves[g, 1, there], 4.0)
            part[g, 0, span] = total
            part[g, 1, span] = square
        for kind in range(4):
            stat(kind, c, mine).start()

    def arrived(kind, c, mine):
        if mine:
            return ring[kind, 0, c, pl.ds(0, half // 2)], ring[kind, 1, c, pl.ds(0, half // 2)]
        return ring[kind, 0, c], ring[kind, 1, c]

    def hand_on_sums(c, mine):
        one = 8.0 if mine else 4.0
        for kind, owner, span in ((0, x_after, plus(c, mine)), (1, x_before, minus(c, mine))):
            stat_arrival(kind, c, mine).wait_recv()
            total, square = merge(part[owner, 0, span], part[owner, 1, span], one, *arrived(kind, c, mine), one)
            part[owner, 0, span] = total
            part[owner, 1, span] = square
            stat(4 + kind, c, mine).start()

    def finish(total, square, span):
        full[xq, 0, span] = total * (1.0 / 32.0)
        full[xq, 1, span] = lax.rsqrt(square * (1.0 / 32.0) + 0.0001)

    def own_sums(c, mine):
        one = 8.0 if mine else 4.0
        for kind in (2, 3, 4, 5):
            stat_arrival(kind, c, mine).wait_recv()
        for near, far, span in ((3, 4, plus(c, mine)), (2, 5, minus(c, mine))):
            total, square = merge(part[xq, 0, span], part[xq, 1, span], one, *arrived(near, c, mine), one)
            total, square = merge(total, square, 2 * one, *arrived(far, c, mine), 2 * one)
            if mine:
                finish(total, square, span)
            else:
                part[xq, 0, span] = total
                part[xq, 1, span] = square
        if mine:
            stat(7, c, mine).start()
            stat(8, c, mine).start()
        else:
            stat(6, c, mine).start()

    def join_partner(c, mine):
        stat_arrival(6, c, mine).wait_recv()
        for offset in (0, half):
            span, there = pl.ds(c * chunk + offset, half), pl.ds((c - FIRST) * chunk + offset, half)
            finish(*merge(part[xq, 0, span], part[xq, 1, span], 16.0, across[0, there], across[1, there], 16.0), span)
        stat(7, c, mine).start()
        stat(8, c, mine).start()

    def hand_on_results(c, mine):
        stat_arrival(7, c, mine).wait_recv()
        stat(9, c, mine).start()
        stat_arrival(8, c, mine).wait_recv()
        stat(10, c, mine).start()

    def collect(c, mine):
        stat_arrival(9, c, mine).wait_recv()
        stat_arrival(10, c, mine).wait_recv()
        if mine:
            stat(11, c, mine).start()

    def last_half(c, mine):
        stat_arrival(11, c, mine).wait_recv()

    rounds = {
        True: (begin, join_halves, hand_on_sums, own_sums, hand_on_results, collect, last_half),
        False: (begin, hand_on_sums, own_sums, join_partner, hand_on_results, collect),
    }
    bounds = {True: (0, FIRST), False: (FIRST, NC)}

    @pl.loop(0, NC + 6)
    def _(k):
        @pl.when(k < NC)
        def _():
            compute(STEPS - 1, k)

        for delay in range(7):
            for mine in (True, False):
                low, high = bounds[mine]
                if delay < len(rounds[mine]) and low < high:
                    @pl.when(jnp.logical_and(k >= low + delay, k < high + delay))
                    def _():
                        rounds[mine][delay](k - delay, mine)

    @pl.loop(0, NC)
    def _(c):
        for side in range(2):
            @pl.when(has["x", side])
            def _():
                x_copy((STEPS - 1) % 2, c, side).wait_send()

            @pl.when(has["z", side])
            def _():
                z_copy((STEPS - 1) % 2, c, side).wait_send()

        for side in range(2):
            @pl.when(jnp.logical_and(carries[side], odd(c)))
            def _():
                for step in range(STEPS):
                    pass_on(step, c, side).wait_send()

        for mine in (True, False):
            low, high = bounds[mine]

            @pl.when(jnp.logical_and(c >= low, c < high))
            def _():
                for kind in range(12 if mine else 11):
                    stat(kind, c, mine).wait_send()


    for side in range(2):
        @pl.when(has["y", side])
        def _():
            y_copy((STEPS - 1) % 2, side).wait_send()


def finish_kernel(u_ref, f_ref, norm_ref, end_ref, sem):
    step = pl.program_id(0)
    tile = norm_ref.shape[0]

    def out(piece):
        span = pl.ds(piece * tile, tile)
        return pltpu.make_async_copy(u_ref.at[span], end_ref.at[span], sem.at[piece])

    out(step).start()

    @pl.loop(0, tile)
    def _(r):
        y = step * tile + r
        for x in range(u_ref.shape[1]):
            for g in range(4):
                band = slice(8 * g, 8 * g + 8)
                norm_ref[r, x, band] = (u_ref[y, x, band] - f_ref[g, 0, y]) * f_ref[g, 1, y]

    @pl.when(step == pl.num_programs(0) - 1)
    def _():
        @pl.loop(0, pl.num_programs(0))
        def _(piece):
            out(piece).wait()


def body(u, k, q):
    rows, cols, height, lanes = u.shape
    dma = pltpu.SemaphoreType.DMA
    moved, stats = pl.pallas_call(
        main_kernel,
        out_shape=(
            pltpu.VMEM(u.shape, F32),
            pltpu.VMEM((4, 2, rows, 8, lanes), F32),
        ),
        in_specs=[pl.BlockSpec(memory_space=pl.ANY)] * 3,
        out_specs=[pl.BlockSpec(memory_space=pltpu.VMEM)] * 2,
        scratch_shapes=[
            pltpu.VMEM((2, rows + 2, cols + 2, height, lanes), F32),
            pltpu.VMEM(u.shape, F32),
            pltpu.VMEM((2, 2, rows, cols, lanes), F32),
            pltpu.VMEM((2, 2, rows, cols, lanes), F32),
            pltpu.VMEM((4, 2, rows, 8, lanes), F32),
            pltpu.VMEM((6, 2, NC, rows // NC // 2, 8, lanes), F32),
            pltpu.VMEM((2, max(NC - FIRST, 1) * (rows // NC), 8, lanes), F32),
            pltpu.VMEM((4, 2, max(FIRST, 1) * (rows // NC // 2), 8, lanes), F32),
            pltpu.VMEM((STEPS, NC // 2, rows // NC, height, lanes), F32),
            dma((3, NC)), dma((STEPS, NC // 2)), dma((STEPS, NC // 2)),
            dma((2, 2, NC)), dma((2, 2, NC)), dma((2, 2, NC)), dma((2, 2, NC)),
            dma((2, 2)), dma((2, 2)), dma((12, NC)), dma((12, NC)),
        ],
        compiler_params=pltpu.CompilerParams(
            collective_id=0, has_side_effects=True, vmem_limit_bytes=49 * 1024 * 1024
        ),
        name="heat_steps",
    )(u, k, q)
    tile = 32
    return pl.pallas_call(
        finish_kernel,
        grid=(rows // tile,),
        out_shape=(jax.ShapeDtypeStruct(u.shape, F32),) * 2,
        in_specs=[pl.BlockSpec(memory_space=pltpu.VMEM)] * 2,
        out_specs=[
            pl.BlockSpec((tile, cols, height, lanes), lambda i: (i, 0, 0, 0)),
            pl.BlockSpec(memory_space=pl.ANY),
        ],
        scratch_shapes=[dma((rows // tile,))],
        compiler_params=pltpu.CompilerParams(vmem_limit_bytes=8 * 1024 * 1024),
        name="centre_and_scale",
    )(moved, stats)


def solution(mesh):
    placed = P("py", "px", "pz", None)
    return jax.shard_map(
        body, mesh=mesh, in_specs=(placed, placed, placed), out_specs=(placed, placed), check_vma=False
    )
```
